32 devices in a mesh: seq: 2 (over core), chan: 4 (over y, x), batch: 4 (over z).
Axes of the slice: x: 2, y: 2, z: 4, core: 2. Of those that a mesh axis runs over, the one named last changes fastest.
Arguments:
- ssm_input: bfloat16 [8192, 4096], P(('batch', 'seq'), 'chan'), parts along dimension 0, may hold values from -6 to 6
- gate_z: bfloat16 [8192, 4096], P(('batch', 'seq'), 'chan'), parts along dimension 0, may hold values from -6 to 6
- proj_forward: bfloat16 [2, 8192, 128], P(None, ('batch', 'seq')), parts along dimension 1, may hold values from -2 to 2
- proj_backward: bfloat16 [2, 8192, 128], P(None, ('batch', 'seq')), parts along dimension 1, may hold values from -2 to 2
- step_raw: float32 [2, 64, 8192], P(None, 'chan', ('batch', 'seq')), parts along dimension 2, may hold values from -3 to 3
- head_params: float32 [2, 2, 64], P(None, None, 'chan'), may hold values from -4 to 1, as said below
- skip_gain: float32 [64], P('chan'), may hold values from 0.25 to 2
- norm_gain: float32 [4096], P('chan'), may hold values from 0.5 to 1.5
- out_weight: bfloat16 [4096, 2048], P(None, 'chan'), may hold values from -0.09375 to 0.09375
Outputs:
- mixed: bfloat16 [8192, 2048], P(('batch', 'seq'), 'chan'), parts along dimension 0
The draws below stay inside these ranges and needn't reach their ends.
There are 4 independent parts, one for each index of `batch`. The reference program is written for one: setup_inputs(seed, part) draws one part's arguments, and reference() takes and returns one part's arrays. A program takes and returns all parts, laid end to end along the dimension named above; an argument that names none is the same for every part. Nothing has to cross between parts.
Inputs may be any that keep to these rules, and one draw needn't show every extreme that they name: `head_params`: index 0 of the second dimension holds positive decay rates, index 1 time-step biases.
All inputs are finite; a program needn't handle non-finite values.
Results may differ from the reference program's by a relative error of at most 0.0085.
Values may be sent and summed in bfloat16 or wider, within the bound.
A program may use at most 128 MiB of HBM per device.

```python
import math
import jax
import jax.numpy as jnp
from jax import lax

DMODEL = 2048
HEADS = 64
HEAD_DIM = 64
NSTATE = 128
SPAN = 256
TOK_DEV = 1024
INNER = 4096
SEQ_LEN = 2048


def draw_head_params(key, part):
    layers = []
    for direction in range(2):
        subkeys = jax.random.split(jax.random.fold_in(key, 11 + direction), 5)
        ranking = jax.random.permutation(subkeys[0], HEADS)
        strong_count = HEADS // 2
        strong = ranking < strong_count
        fast_rate = jnp.exp(jax.random.uniform(subkeys[1], (HEADS,), jnp.float32, math.log(0.025), math.log(0.045)))
        slow_rate = jnp.exp(jax.random.uniform(subkeys[2], (HEADS,), jnp.float32, math.log(2.4), math.log(24.0))) / SEQ_LEN
        fast_bias = jax.random.uniform(subkeys[3], (HEADS,), jnp.float32, -0.5, 0.5)
        slow_bias = jax.random.uniform(subkeys[4], (HEADS,), jnp.float32, -4.0, -3.0)
        decay_rates = jnp.where(strong, fast_rate, slow_rate)
        biases = jnp.where(strong, fast_bias, slow_bias)
        layers.append(jnp.stack([decay_rates, biases]))
    return jnp.stack(layers).astype(jnp.float32)


def draw_step_raw(key, part):
    subkeys = jax.random.split(jax.random.fold_in(key, 29), 2)
    jitter = jnp.clip(0.5 * jax.random.normal(subkeys[0], (2, HEADS, SEQ_LEN), jnp.float32), -1.5, 1.5)
    groups = SEQ_LEN // TOK_DEV
    offsets = jax.random.uniform(subkeys[1], (2, 1, groups), jnp.float32, -1.0, 1.0)
    return (jitter + jnp.repeat(offsets, TOK_DEV, axis=2)).astype(jnp.float32)


def levels(key, shape, shards, low, largest):
    factor_of, own = 1.0, jax.random.fold_in(key, 6)
    for dim, blocks in shards:
        heights = jnp.exp(jax.random.uniform(jax.random.fold_in(own, dim), (blocks,), jnp.float32, low / len(shards), largest / len(shards)))
        factor_of = factor_of * jnp.repeat(heights, shape[dim] // blocks).reshape([-1 if axis == dim else 1 for axis in range(len(shape))])
    return factor_of


def scatter_about(key, shape, width, reach, shards=(), held_as=jnp.bfloat16):
    result = jax.random.normal(key, shape, jnp.float32) * width
    if len(shards) > 0:
        result = levels(key, shape, shards, -0.22, 0.18) * result
    return jnp.clip(result, min=-reach, max=reach).astype(held_as)


def setup_inputs(seed: int = 0, part: int = 0) -> dict:
    arg_keys = jax.random.split(jax.random.key(seed), 10)
    own_keys = jax.random.split(jax.random.fold_in(arg_keys[9], part), 10)
    ssm_input = scatter_about(own_keys[0], (SEQ_LEN, INNER), 1.0, 6.0, ((0, 2), (1, 4)))
    gate_z = scatter_about(own_keys[1], (SEQ_LEN, INNER), 1.0, 6.0, ((0, 2), (1, 4)))
    proj_forward = scatter_about(own_keys[2], (2, SEQ_LEN, NSTATE), 0.3, 2.0, ((1, 2),))
    proj_backward = scatter_about(own_keys[3], (2, SEQ_LEN, NSTATE), 0.3, 2.0, ((1, 2),))
    step_raw = draw_step_raw(jax.random.fold_in(jax.random.fold_in(arg_keys[9], part), 71), part)
    head_params = draw_head_params(jax.random.fold_in(arg_keys[9], 71), part)
    skip_gain = jnp.clip(jnp.exp(math.log(2.0) - 2.0794415 * jax.random.uniform(arg_keys[6], (HEADS,), jnp.float32) ** levels(arg_keys[6], (HEADS,), ((0, 4),), -0.2, 0.2)), 0.25, 2.0)
    norm_gain = jnp.clip(0.5 + 1.0 * jax.random.uniform(arg_keys[7], (INNER,), jnp.float32) ** levels(arg_keys[7], (INNER,), ((0, 4),), -0.2, 0.2), 0.5, 1.5)
    out_weight = scatter_about(arg_keys[8], (INNER, DMODEL), INNER ** -0.5, 0.09375, ((1, 4),))
    return dict(ssm_input=ssm_input, gate_z=gate_z, proj_forward=proj_forward, proj_backward=proj_backward, step_raw=step_raw, head_params=head_params, skip_gain=skip_gain, norm_gain=norm_gain, out_weight=out_weight)


def ssd(values, b_rows, c_rows, steps, rates):
    length = values.shape[0]
    blocks = length // SPAN
    blocks_x = values.reshape(blocks, SPAN, HEADS, HEAD_DIM)
    blocks_b = b_rows.reshape(blocks, SPAN, NSTATE)
    blocks_c = c_rows.reshape(blocks, SPAN, NSTATE)
    blocks_dt = steps.reshape(HEADS, blocks, SPAN).transpose(1, 0, 2)
    lower_mask = jnp.tril(jnp.ones((SPAN, SPAN), dtype=bool))

    def advance(entering, inputs):
        block_x, block_b, block_c, block_dt = inputs
        cumlog = jnp.cumsum(-rates[:, None] * block_dt, axis=1)
        scores = jnp.dot(block_c, block_b.T, preferred_element_type=jnp.float32)
        log_gaps = cumlog[:, :, None] - cumlog[:, None, :]
        decays = jnp.where(lower_mask, jnp.exp(jnp.where(lower_mask, log_gaps, 0.0)), 0.0)
        weights = (scores[None] * decays * block_dt[:, None, :]).astype(jnp.bfloat16)
        intra_out = jnp.einsum('hts,shp->thp', weights.astype(jnp.float32), block_x.astype(jnp.float32))
        in_weights = jnp.exp(cumlog[:, -1:] - cumlog) * block_dt
        b_weighted = (block_b.astype(jnp.float32)[None] * in_weights[:, :, None]).astype(jnp.bfloat16)
        block_state = jnp.einsum('shp,hsn->hpn', block_x.astype(jnp.float32), b_weighted.astype(jnp.float32))
        inter = jnp.einsum('tn,hpn->thp', block_c.astype(jnp.float32), entering, precision=lax.Precision.HIGHEST)
        inter = inter * jnp.exp(cumlog).T[:, :, None]
        following = jnp.exp(cumlog[:, -1])[:, None, None] * entering + block_state
        return (following, intra_out + inter)
    initial = jnp.zeros((HEADS, HEAD_DIM, NSTATE), jnp.float32)
    _, outputs = lax.scan(advance, initial, (blocks_x, blocks_b, blocks_c, blocks_dt))
    return outputs.reshape(length, HEADS * HEAD_DIM)

def reference(ssm_input, gate_z, proj_forward, proj_backward, step_raw, head_params, skip_gain, norm_gain, out_weight):
    steps_fwd = jax.nn.softplus(step_raw[0] + head_params[0, 1][:, None])
    steps_bwd = jax.nn.softplus(step_raw[1] + head_params[1, 1][:, None])
    forward_out = ssd(ssm_input, proj_forward[0], proj_forward[1], steps_fwd, head_params[0, 0])
    backward_out = ssd(ssm_input[::-1], proj_backward[0][::-1], proj_backward[1][::-1], steps_bwd[:, ::-1], head_params[1, 0])[::-1]
    frames = ssm_input.shape[0]
    skipped = (ssm_input.reshape(frames, HEADS, HEAD_DIM).astype(jnp.float32) * skip_gain[:, None]).reshape(frames, INNER)
    gated = (forward_out + backward_out + skipped) * jax.nn.silu(gate_z.astype(jnp.float32))
    scale = lax.rsqrt(lax.optimization_barrier(jnp.sum(gated * gated, axis=1)) / INNER + 1.0)
    normed = (gated * scale[:, None] * norm_gain).astype(jnp.bfloat16)
    return jnp.dot(normed, out_weight, preferred_element_type=jnp.float32).astype(jnp.bfloat16)
```

```python
import functools

import jax
import jax.numpy as jnp
from jax import lax
from jax.experimental import pallas as pl
from jax.experimental.pallas import tpu as pltpu
from jax.sharding import PartitionSpec as P

Q = 128
LOG2E = 1.4426950408889634
F32, BF16 = jnp.float32, jnp.bfloat16


def nn(a, b):
    return lax.dot_general(a, b, (((1,), (0,)), ((), ())), preferred_element_type=F32)


def nt(a, b):
    return lax.dot_general(a, b, (((1,), (1,)), ((), ())), preferred_element_type=F32)


def tn(a, b):
    return lax.dot_general(a, b, (((0,), (0,)), ((), ())), preferred_element_type=F32)


def rates_of(raw, hp_ref, heads):
    v = raw + hp_ref[:, 1:2]
    dt = jnp.maximum(v, 0.0) + jnp.log1p(jnp.exp(-jnp.abs(v)))
    l2 = (-LOG2E) * hp_ref[:, 0:1] * dt
    r = lax.broadcasted_iota(jnp.int32, (Q, Q), 0)
    t = lax.broadcasted_iota(jnp.int32, (Q, Q), 1)
    up = (r <= t).astype(F32)
    down = (r >= t).astype(F32)
    cf = jnp.dot(l2, up, preferred_element_type=F32, precision=lax.Precision.HIGHEST)
    cb = jnp.dot(l2, down, preferred_element_type=F32, precision=lax.Precision.HIGHEST)
    forward = lax.broadcasted_iota(jnp.int32, l2.shape, 0) < heads
    cum = jnp.where(forward, cf, cb)
    total = jnp.sum(l2, axis=1, keepdims=True)
    return dt, cum, total, jnp.log2(dt) - cum


def columns_of(rows):
    used = sum(r.shape[0] for r in rows)
    if used < 128:
        rows = rows + [jnp.zeros((128 - used, Q), F32)]
    return jnp.concatenate(rows, axis=0).T


def halves(cols):
    hi = cols.astype(BF16)
    lo = (cols - hi.astype(F32)).astype(BF16)
    return jnp.concatenate([hi, lo], axis=1)


def fill_spread(spread_ref, groups, heads, width):
    for k, group in enumerate(groups):
        shape = spread_ref.shape[1:]
        j = lax.broadcasted_iota(jnp.int32, shape, 0) % 128
        head = lax.broadcasted_iota(jnp.int32, shape, 1) // width
        spread_ref[k] = jnp.where(j == group * heads + head, 1.0, 0.0).astype(BF16)


def states_kernel(
    heads, width, x_ref, bf_ref, bb_ref, raw_ref, hp_ref,
    entf_ref, entb_ref, dec_ref, end_ref, endb_ref, tot_ref, sf, sb, df, db, spread,
):
    blocks = x_ref.shape[0] // Q
    fill_spread(spread, (0, 1, 2, 3), heads, width)
    sf[...] = jnp.zeros_like(sf)
    sb[...] = jnp.zeros_like(sb)
    df[...] = jnp.ones_like(df)
    db[...] = jnp.ones_like(db)

    def step(i, _):
        k = blocks - 1 - i
        at_f = pl.multiple_of(i * Q, Q)
        at_b = pl.multiple_of(k * Q, Q)
        raw = jnp.concatenate(
            [raw_ref[:, pl.ds(at_f, Q)][:heads], raw_ref[:, pl.ds(at_b, Q)][heads:]], axis=0
        )
        dt, cum, total, rowt = rates_of(raw, hp_ref, heads)
        gain = jnp.broadcast_to(jnp.exp2(total), cum.shape)
        cols = halves(columns_of([jnp.exp2(total + rowt), gain]))
        for at, block, b_ref, ent, state, dec, place in (
            (at_f, i, bf_ref, entf_ref, sf, df, 0),
            (at_b, k, bb_ref, entb_ref, sb, db, 1),
        ):
            ent[block] = state[...].astype(BF16)
            dec_ref[block, pl.ds(8 * place, 8), :] = dec[...]
            weigh = nn(cols, spread[place])
            xw = (x_ref[pl.ds(at, Q), :].astype(F32) * weigh).astype(BF16)
            decay = nn(cols[:16], spread[2 + place])[:8]
            state[...] = state[...] * decay[:1] + tn(b_ref[pl.ds(at, Q), :], xw)
            dec[...] = dec[...] * decay
        return 0

    lax.fori_loop(0, blocks, step, 0)
    end_ref[...] = sf[...].astype(BF16)
    endb_ref[...] = sb[...].astype(BF16)
    tot_ref[pl.ds(0, 8), :] = df[...]
    tot_ref[pl.ds(8, 8), :] = db[...]


def outputs_kernel(
    heads, width, x_ref, z_ref, pf_ref, pb_ref, raw_ref, hp_ref, skip_ref, gain_ref,
    entf_ref, entb_ref, dec_ref, cf_ref, cb_ref, g_ref, sq_ref, spread, base,
):
    @pl.when(pl.program_id(0) == 0)
    def _():
        fill_spread(spread, (2, 3, 5), heads, width)

    dt, cum, total, rowt = rates_of(raw_ref[...], hp_ref, heads)
    cols = columns_of([cum, jnp.exp2(cum), dt])
    b_f, c_f, b_b, c_b = pf_ref[0], pf_ref[1], pb_ref[0], pb_ref[1]
    lane = lax.broadcasted_iota(jnp.int32, (Q, 128), 1)
    diag = jnp.sum(b_b.astype(F32) * c_b.astype(F32), axis=1, keepdims=True)
    here = (lane >= 5 * heads) & (lane < 6 * heads)
    wide = halves(jnp.where(here, cols * diag + skip_ref[...], cols))
    dec = dec_ref[0]
    ent_f = (entf_ref[0].astype(F32) + dec[0:1] * cf_ref[...].astype(F32)).astype(BF16)
    ent_b = (entb_ref[0].astype(F32) + dec[8:9] * cb_ref[...].astype(F32)).astype(BF16)
    base[...] = nn(wide, spread[0]) * nn(c_f, ent_f)
    base[...] += nn(wide, spread[1]) * nn(c_b, ent_b)
    base[...] += nn(wide, spread[2]) * x_ref[...].astype(F32)

    t = lax.broadcasted_iota(jnp.int32, (Q, Q), 0)
    s = lax.broadcasted_iota(jnp.int32, (Q, Q), 1)
    lower = s <= t
    scores = jnp.where(lower, nt(c_f, b_f), nt(c_b, b_b))
    per = 128 // width
    squares = jnp.zeros((Q, 128), F32)
    for group in range(heads // per):
        lanes = slice(group * 128, (group + 1) * 128)
        x = x_ref[:, lanes]
        weights, values = [], []
        for k in range(per):
            h = group * per + k
            gap_f = cols[:, h : h + 1] + rowt[h : h + 1, :]
            gap_b = cols[:, heads + h : heads + h + 1] + rowt[heads + h : heads + h + 1, :]
            weights.append((scores * jnp.exp2(jnp.where(lower, gap_f, gap_b))).astype(BF16))
            own = (lane >= k * width) & (lane < (k + 1) * width)
            values.append(jnp.where(own, x, jnp.zeros_like(x)))
        intra = nn(jnp.concatenate(weights, axis=1), jnp.concatenate(values, axis=0))
        z = z_ref[:, lanes].astype(F32)
        gated = (base[:, lanes] + intra) * (z / (1.0 + jnp.exp(-z)))
        squares += gated * gated
        g_ref[:, lanes] = (gated * gain_ref[:, lanes]).astype(BF16)
    sums = jnp.sum(squares.T, axis=0, keepdims=True)
    sq_ref[...] = jnp.broadcast_to(sums, sq_ref.shape)


def body(
    ssm_input, gate_z, proj_forward, proj_backward, step_raw, head_params,
    skip_gain, norm_gain, out_weight,
):
    frames, inner = ssm_input.shape
    heads = step_raw.shape[1]
    width = inner // heads
    state = proj_forward.shape[2]
    blocks = frames // Q
    features = out_weight.shape[1]
    n_chan, n_seq = lax.axis_size("chan"), lax.axis_size("seq")
    chan, seq = lax.axis_index("chan"), lax.axis_index("seq")
    all_channels = inner * n_chan

    paired = n_chan & (n_chan - 1) == 0

    def partner(i, k):
        return i ^ k if paired else (i + k) % n_chan

    def source(i, k):
        return i ^ k if paired else (i + n_chan - k) % n_chan

    share = inner // n_seq
    pieces = {}
    for k in range(1, n_chan):
        start = partner(chan, k) * inner + seq * share
        part = lax.dynamic_slice(out_weight, (start, 0), (share, features))
        pieces[k] = lax.ppermute(part, "chan", [(i, partner(i, k)) for i in range(n_chan)])
    weights = {0: lax.dynamic_slice(out_weight, (chan * inner, 0), (inner, features))}
    for k in range(1, n_chan):
        whole = jnp.zeros((inner, features), out_weight.dtype)
        whole = lax.dynamic_update_slice(whole, pieces[k], (seq * share, 0))
        for j in range(1, n_seq):
            got = lax.ppermute(pieces[k], "seq", [(i, (i + j) % n_seq) for i in range(n_seq)])
            whole = lax.dynamic_update_slice(whole, got, (((seq + n_seq - j) % n_seq) * share, 0))
        weights[k] = whole

    raw = step_raw.reshape(2 * heads, frames)
    params = jnp.stack([head_params[:, 0].reshape(-1), head_params[:, 1].reshape(-1)], axis=1)
    skip_row = jnp.zeros((1, 128), F32)
    skip_row = lax.dynamic_update_slice(skip_row, skip_gain[None], (0, 5 * heads))
    gain_row = norm_gain[None]

    ent_f, ent_b, dec, end_f, end_b, tot = pl.pallas_call(
        functools.partial(states_kernel, heads, width),
        out_shape=(
            jax.ShapeDtypeStruct((blocks, state, inner), BF16),
            jax.ShapeDtypeStruct((blocks, state, inner), BF16),
            jax.ShapeDtypeStruct((blocks, 16, inner), F32),
            jax.ShapeDtypeStruct((state, inner), BF16),
            jax.ShapeDtypeStruct((state, inner), BF16),
            jax.ShapeDtypeStruct((16, inner), F32),
        ),
        scratch_shapes=[
            pltpu.VMEM((state, inner), F32),
            pltpu.VMEM((state, inner), F32),
            pltpu.VMEM((8, inner), F32),
            pltpu.VMEM((8, inner), F32),
            pltpu.VMEM((4, 256, inner), BF16),
        ],
        compiler_params=pltpu.CompilerParams(vmem_limit_bytes=40 * 2**20),
        cost_estimate=pl.CostEstimate(
            flops=4 * 10**9, bytes_accessed=8 * 2**20, transcendentals=0
        ),
        name="scan_states",
    )(ssm_input, proj_forward[0], proj_backward[0], raw, params)

    def carried(end, decay, step):
        pairs = [(i, i + step) for i in range(n_seq) if 0 <= i + step < n_seq]
        out = lax.ppermute(end, "seq", pairs)
        for _ in range(n_seq - 2):
            new = (end.astype(F32) + decay * out.astype(F32)).astype(BF16)
            out = lax.ppermute(new, "seq", pairs)
        return out

    carry_f = carried(end_f, tot[0:1], 1)
    carry_b = carried(end_b, tot[8:9], -1)

    chunks = 2 if blocks % 2 == 0 else 1
    count = blocks // chunks
    received = []
    for chunk in range(chunks):
        at = chunk * count
        rows = lambda i, at=at: (i + at, 0)
        rows3 = lambda i, at=at: (0, i + at, 0)
        block3 = lambda i, at=at: (i + at, 0, 0)
        same = lambda i: (0, 0)
        gated, sums = pl.pallas_call(
            functools.partial(outputs_kernel, heads, width),
            grid=(count,),
            in_specs=[
                pl.BlockSpec((Q, inner), rows),
                pl.BlockSpec((Q, inner), rows),
                pl.BlockSpec((2, Q, state), rows3),
                pl.BlockSpec((2, Q, state), rows3),
                pl.BlockSpec((2 * heads, Q), lambda i, at=at: (0, i + at)),
                pl.BlockSpec((2 * heads, 2), same),
                pl.BlockSpec((1, 128), same),
                pl.BlockSpec((1, inner), same),
                pl.BlockSpec((1, state, inner), block3),
                pl.BlockSpec((1, state, inner), block3),
                pl.BlockSpec((1, 16, inner), block3),
                pl.BlockSpec((state, inner), same),
                pl.BlockSpec((state, inner), same),
            ],
            out_specs=(
                pl.BlockSpec((Q, inner), lambda i: (i, 0)),
                pl.BlockSpec((8, Q), lambda i: (0, i)),
            ),
            out_shape=(
                jax.ShapeDtypeStruct((count * Q, inner), BF16),
                jax.ShapeDtypeStruct((8, count * Q), F32),
            ),
            scratch_shapes=[pltpu.VMEM((3, 256, inner), BF16), pltpu.VMEM((Q, inner), F32)],
            compiler_params=pltpu.CompilerParams(
                vmem_limit_bytes=40 * 2**20, dimension_semantics=("arbitrary",)
            ),
            cost_estimate=pl.CostEstimate(
                flops=4 * 10**9, bytes_accessed=8 * 2**20, transcendentals=0
            ),
            name="scan_outputs",
        )(
            ssm_input, gate_z, proj_forward, proj_backward, raw, params, skip_row, gain_row,
            ent_f, ent_b, dec, carry_f, carry_b,
        )
        sums = sums[0:1]
        squares = sums
        got = []
        for k in range(1, n_chan):
            perm = [(i, partner(i, k)) for i in range(n_chan)]
            kin = k if paired else n_chan - k
            part = jnp.dot(gated, weights[kin], preferred_element_type=F32).astype(BF16)
            got.append(lax.ppermute(part, "chan", perm))
            squares = squares + lax.ppermute(sums, "chan", perm)
        own = jnp.dot(gated, weights[0], preferred_element_type=F32)
        for part in got:
            own = own + part.astype(F32)
        scale = lax.rsqrt(squares[0] / all_channels + 1.0)
        received.append((own * scale[:, None]).astype(BF16))
    return jnp.concatenate(received, axis=0)


def solution(mesh):
    in_specs = (
        P(("batch", "seq"), "chan"),
        P(("batch", "seq"), "chan"),
        P(None, ("batch", "seq"), None),
        P(None, ("batch", "seq"), None),
        P(None, "chan", ("batch", "seq")),
        P(None, None, "chan"),
        P("chan"),
        P("chan"),
        P(None, "chan"),
    )
    out_specs = P(("batch", "seq"), "chan")
    return jax.shard_map(body, mesh=mesh, in_specs=in_specs, out_specs=out_specs, check_vma=False)
```

```python
import functools

import jax
import jax.numpy as jnp
from jax import lax
from jax.experimental import pallas as pl
from jax.experimental.pallas import tpu as pltpu
from jax.sharding import PartitionSpec as P


Q = 128
LOG2E = 1.4426950408889634
F32, BF16 = jnp.float32, jnp.bfloat16


def nn(a, b):
    return lax.dot_general(a, b, (((1,), (0,)), ((), ())), preferred_element_type=F32)


def nt(a, b):
    return lax.dot_general(a, b, (((1,), (1,)), ((), ())), preferred_element_type=F32)


def tn(a, b):
    return lax.dot_general(a, b, (((0,), (0,)), ((), ())), preferred_element_type=F32)


def rates_of(raw, hp_ref, heads):
    v = raw + hp_ref[:, 1:2]
    dt = jnp.maximum(v, 0.0) + jnp.log1p(jnp.exp(-jnp.abs(v)))
    l2 = (-LOG2E) * hp_ref[:, 0:1] * dt
    r = lax.broadcasted_iota(jnp.int32, (Q, Q), 0)
    t = lax.broadcasted_iota(jnp.int32, (Q, Q), 1)
    up = (r <= t).astype(F32)
    down = (r >= t).astype(F32)
    cf = jnp.dot(l2, up, preferred_element_type=F32, precision=lax.Precision.HIGHEST)
    cb = jnp.dot(l2, down, preferred_element_type=F32, precision=lax.Precision.HIGHEST)
    forward = lax.broadcasted_iota(jnp.int32, l2.shape, 0) < heads
    cum = jnp.where(forward, cf, cb)
    total = jnp.sum(l2, axis=1, keepdims=True)
    return dt, cum, total, jnp.log2(dt) - cum


def columns_of(rows):
    used = sum(r.shape[0] for r in rows)
    if used < 128:
        rows = rows + [jnp.zeros((128 - used, Q), F32)]
    return jnp.concatenate(rows, axis=0).T


def halves(cols):
    hi = cols.astype(BF16)
    lo = (cols - hi.astype(F32)).astype(BF16)
    return jnp.concatenate([hi, lo], axis=1)


def fill_spread(spread_ref, groups, heads, width):
    for k, group in enumerate(groups):
        shape = spread_ref.shape[1:]
        j = lax.broadcasted_iota(jnp.int32, shape, 0) % 128
        head = lax.broadcasted_iota(jnp.int32, shape, 1) // width
        spread_ref[k] = jnp.where(j == group * heads + head, 1.0, 0.0).astype(BF16)


def states_kernel(
    heads, width, x_ref, bf_ref, bb_ref, raw_ref, hp_ref,
    entf_ref, entb_ref, dec_ref, end_ref, endb_ref, tot_ref, sf, sb, df, db, spread,
):
    blocks = x_ref.shape[0] // Q
    fill_spread(spread, (0, 1, 2, 3), heads, width)
    sf[...] = jnp.zeros_like(sf)
    sb[...] = jnp.zeros_like(sb)
    df[...] = jnp.ones_like(df)
    db[...] = jnp.ones_like(db)

    def step(i, _):
        k = blocks - 1 - i
        at_f = pl.multiple_of(i * Q, Q)
        at_b = pl.multiple_of(k * Q, Q)
        raw = jnp.concatenate(
            [raw_ref[:, pl.ds(at_f, Q)][:heads], raw_ref[:, pl.ds(at_b, Q)][heads:]], axis=0
        )
        _, cum, total, rowt = rates_of(raw, hp_ref, heads)
        gain = jnp.broadcast_to(jnp.exp2(total), cum.shape)
        cols = halves(columns_of([jnp.exp2(total + rowt), gain]))
        for at, block, b_ref, ent, state, dec, place in (
            (at_f, i, bf_ref, entf_ref, sf, df, 0),
            (at_b, k, bb_ref, entb_ref, sb, db, 1),
        ):
            ent[block] = state[...].astype(BF16)
            dec_ref[block, pl.ds(8 * place, 8), :] = dec[...]
            weigh = nn(cols, spread[place])
            xw = (x_ref[pl.ds(at, Q), :].astype(F32) * weigh).astype(BF16)
            decay = nn(cols[:16], spread[2 + place])[:8]
            state[...] = state[...] * decay[:1] + tn(b_ref[pl.ds(at, Q), :], xw)
            dec[...] = dec[...] * decay
        return 0

    lax.fori_loop(0, blocks, step, 0)
    end_ref[...] = sf[...].astype(BF16)
    endb_ref[...] = sb[...].astype(BF16)
    tot_ref[pl.ds(0, 8), :] = df[...]
    tot_ref[pl.ds(8, 8), :] = db[...]


def outputs_kernel(
    heads, width, x_ref, z_ref, pf_ref, pb_ref, raw_ref, hp_ref, skip_ref, gain_ref,
    entf_ref, entb_ref, dec_ref, cf_ref, cb_ref, g_ref, sq_ref, spread, base,
):
    @pl.when(pl.program_id(0) == 0)
    def _():
        fill_spread(spread, (2, 3, 5), heads, width)

    dt, cum, _, rowt = rates_of(raw_ref[...], hp_ref, heads)
    cols = columns_of([cum, jnp.exp2(cum), dt])
    b_f, c_f, b_b, c_b = pf_ref[0], pf_ref[1], pb_ref[0], pb_ref[1]
    lane = lax.broadcasted_iota(jnp.int32, (Q, 128), 1)
    diag = jnp.sum(b_b.astype(F32) * c_b.astype(F32), axis=1, keepdims=True)
    here = (lane >= 5 * heads) & (lane < 6 * heads)
    wide = halves(jnp.where(here, cols * diag + skip_ref[...], cols))
    dec = dec_ref[0]
    ent_f = (entf_ref[0].astype(F32) + dec[0:1] * cf_ref[...].astype(F32)).astype(BF16)
    ent_b = (entb_ref[0].astype(F32) + dec[8:9] * cb_ref[...].astype(F32)).astype(BF16)
    base[...] = nn(wide, spread[0]) * nn(c_f, ent_f)
    base[...] += nn(wide, spread[1]) * nn(c_b, ent_b)
    base[...] += nn(wide, spread[2]) * x_ref[...].astype(F32)

    t = lax.broadcasted_iota(jnp.int32, (Q, Q), 0)
    s = lax.broadcasted_iota(jnp.int32, (Q, Q), 1)
    lower = s <= t
    scores = jnp.where(lower, nt(c_f, b_f), nt(c_b, b_b))
    per = 128 // width
    squares = jnp.zeros((Q, 128), F32)
    for group in range(heads // per):
        lanes = slice(group * 128, (group + 1) * 128)
        x = x_ref[:, lanes]
        weights, values = [], []
        for k in range(per):
            h = group * per + k
            gap_f = cols[:, h : h + 1] + rowt[h : h + 1, :]
            gap_b = cols[:, heads + h : heads + h + 1] + rowt[heads + h : heads + h + 1, :]
            weights.append((scores * jnp.exp2(jnp.where(lower, gap_f, gap_b))).astype(BF16))
            own = (lane >= k * width) & (lane < (k + 1) * width)
            values.append(jnp.where(own, x, jnp.zeros_like(x)))
        intra = nn(jnp.concatenate(weights, axis=1), jnp.concatenate(values, axis=0))
        z = z_ref[:, lanes].astype(F32)
        gated = (base[:, lanes] + intra) * (z / (1.0 + jnp.exp(-z)))
        squares += gated * gated
        g_ref[:, lanes] = (gated * gain_ref[:, lanes]).astype(BF16)
    sums = jnp.sum(squares.T, axis=0, keepdims=True)
    sq_ref[...] = jnp.broadcast_to(sums, sq_ref.shape)


def body(
    ssm_input, gate_z, proj_forward, proj_backward, step_raw, head_params,
    skip_gain, norm_gain, out_weight,
):
    frames, inner = ssm_input.shape
    heads = step_raw.shape[1]
    width = inner // heads
    state = proj_forward.shape[2]
    blocks = frames // Q
    features = out_weight.shape[1]
    n_chan, n_seq = lax.axis_size("chan"), lax.axis_size("seq")
    chan, seq = lax.axis_index("chan"), lax.axis_index("seq")
    all_channels = inner * n_chan

    assert n_chan & (n_chan - 1) == 0

    share = inner // n_seq
    pieces = {}
    for k in range(1, n_chan):
        start = (chan ^ k) * inner + seq * share
        part = lax.dynamic_slice(out_weight, (start, 0), (share, features))
        pieces[k] = lax.ppermute(part, "chan", [(i, i ^ k) for i in range(n_chan)])
    weights = {0: lax.dynamic_slice(out_weight, (chan * inner, 0), (inner, features))}
    for k in range(1, n_chan):
        whole = jnp.zeros((inner, features), out_weight.dtype)
        whole = lax.dynamic_update_slice(whole, pieces[k], (seq * share, 0))
        for j in range(1, n_seq):
            got = lax.ppermute(pieces[k], "seq", [(i, (i + j) % n_seq) for i in range(n_seq)])
            whole = lax.dynamic_update_slice(whole, got, (((seq + n_seq - j) % n_seq) * share, 0))
        weights[k] = whole

    raw = step_raw.reshape(2 * heads, frames)
    params = jnp.stack([head_params[:, 0].reshape(-1), head_params[:, 1].reshape(-1)], axis=1)
    skip_row = jnp.zeros((1, 128), F32)
    skip_row = lax.dynamic_update_slice(skip_row, skip_gain[None], (0, 5 * heads))
    gain_row = norm_gain[None]

    states = pl.pallas_call(
        functools.partial(states_kernel, heads, width),
        out_shape=(
            jax.ShapeDtypeStruct((blocks, state, inner), BF16),
            jax.ShapeDtypeStruct((blocks, state, inner), BF16),
            jax.ShapeDtypeStruct((blocks, 16, inner), F32),
            jax.ShapeDtypeStruct((state, inner), BF16),
            jax.ShapeDtypeStruct((state, inner), BF16),
            jax.ShapeDtypeStruct((16, inner), F32),
        ),
        scratch_shapes=[
            pltpu.VMEM((state, inner), F32),
            pltpu.VMEM((state, inner), F32),
            pltpu.VMEM((8, inner), F32),
            pltpu.VMEM((8, inner), F32),
            pltpu.VMEM((4, 256, inner), BF16),
        ],
        compiler_params=pltpu.CompilerParams(vmem_limit_bytes=60 * 2**20),
        cost_estimate=pl.CostEstimate(
            flops=4 * 10**9, bytes_accessed=8 * 2**20, transcendentals=0
        ),
        name="scan_states",
    )
    ent_f, ent_b, dec, end_f, end_b, tot = states(
        ssm_input, proj_forward[0], proj_backward[0], raw, params
    )

    def carried(end, decay, step):
        pairs = [(i, i + step) for i in range(n_seq) if 0 <= i + step < n_seq]
        out = lax.ppermute(end, "seq", pairs)
        for _ in range(n_seq - 2):
            new = (end.astype(F32) + decay * out.astype(F32)).astype(BF16)
            out = lax.ppermute(new, "seq", pairs)
        return out

    carry_f = carried(end_f, tot[0:1], 1)
    carry_b = carried(end_b, tot[8:9], -1)

    chunks = 2 if blocks % 2 == 0 else 1
    count = blocks // chunks
    owned, squares = [], []
    for chunk in range(chunks):
        at = chunk * count
        rows = lambda i, at=at: (i + at, 0)
        rows3 = lambda i, at=at: (0, i + at, 0)
        block3 = lambda i, at=at: (i + at, 0, 0)
        same = lambda i: (0, 0)
        outputs = pl.pallas_call(
            functools.partial(outputs_kernel, heads, width),
            grid=(count,),
            in_specs=[
                pl.BlockSpec((Q, inner), rows),
                pl.BlockSpec((Q, inner), rows),
                pl.BlockSpec((2, Q, state), rows3),
                pl.BlockSpec((2, Q, state), rows3),
                pl.BlockSpec((2 * heads, Q), lambda i, at=at: (0, i + at)),
                pl.BlockSpec((2 * heads, 2), same),
                pl.BlockSpec((1, 128), same),
                pl.BlockSpec((1, inner), same),
                pl.BlockSpec((1, state, inner), block3),
                pl.BlockSpec((1, state, inner), block3),
                pl.BlockSpec((1, 16, inner), block3),
                pl.BlockSpec((state, inner), same),
                pl.BlockSpec((state, inner), same),
            ],
            out_specs=(
                pl.BlockSpec((Q, inner), lambda i: (i, 0)),
                pl.BlockSpec((8, Q), lambda i: (0, i)),
            ),
            out_shape=(
                jax.ShapeDtypeStruct((count * Q, inner), BF16),
                jax.ShapeDtypeStruct((8, count * Q), F32),
            ),
            scratch_shapes=[pltpu.VMEM((3, 256, inner), BF16), pltpu.VMEM((Q, inner), F32)],
            compiler_params=pltpu.CompilerParams(
                vmem_limit_bytes=60 * 2**20, dimension_semantics=("arbitrary",)
            ),
            cost_estimate=pl.CostEstimate(
                flops=4 * 10**9, bytes_accessed=8 * 2**20, transcendentals=0
            ),
            name="scan_outputs",
        )
        gated, sums = outputs(
            ssm_input, gate_z, proj_forward, proj_backward, raw, params, skip_row, gain_row,
            ent_f, ent_b, dec, carry_f, carry_b,
        )
        bits = [1 << b for b in range(n_chan.bit_length() - 1)]
        bits = bits if chunk % 2 == 0 else bits[::-1]
        parts = {
            r: jnp.dot(gated, weights[r], preferred_element_type=F32)
            for r in range(n_chan)
        }
        for bit in bits:
            perm = [(i, i ^ bit) for i in range(n_chan)]
            going = sorted((r for r in parts if r & bit), reverse=True)
            got = {r ^ bit: lax.ppermute(parts.pop(r).astype(BF16), "chan", perm) for r in going}
            parts = {r: parts[r] + got[r].astype(F32) for r in parts}
        owned.append(parts[0])
        squares.append(sums[0:1])
    squares = jnp.concatenate(squares, axis=1)
    for bit in bits:
        perm = [(i, i ^ bit) for i in range(n_chan)]
        squares = squares + lax.ppermute(squares, "chan", perm)
    scale = lax.rsqrt(squares[0] / all_channels + 1.0)[:, None]
    received = [
        (part * scale[c * count * Q : (c + 1) * count * Q]).astype(BF16)
        for c, part in enumerate(owned)
    ]
    return jnp.concatenate(received, axis=0)


def solution(mesh):
    in_specs = (
        P(("batch", "seq"), "chan"),
        P(("batch", "seq"), "chan"),
        P(None, ("batch", "seq"), None),
        P(None, ("batch", "seq"), None),
        P(None, "chan", ("batch", "seq")),
        P(None, None, "chan"),
        P("chan"),
        P("chan"),
        P(None, "chan"),
    )
    out_specs = P(("batch", "seq"), "chan")
    return jax.shard_map(body, mesh=mesh, in_specs=in_specs, out_specs=out_specs, check_vma=False)
```

```python
import functools

import jax
import jax.numpy as jnp
from jax import lax
from jax.experimental import pallas as pl
from jax.experimental.pallas import tpu as pltpu
from jax.sharding import PartitionSpec as P


Q = 128
LOG2E = 1.4426950408889634
F32, BF16 = jnp.float32, jnp.bfloat16


def nn(a, b):
    return lax.dot_general(a, b, (((1,), (0,)), ((), ())), preferred_element_type=F32)


def nt(a, b):
    return lax.dot_general(a, b, (((1,), (1,)), ((), ())), preferred_element_type=F32)


def tn(a, b):
    return lax.dot_general(a, b, (((0,), (0,)), ((), ())), preferred_element_type=F32)


def rates_of(raw, hp_ref, heads):
    v = raw + hp_ref[:, 1:2]
    dt = jnp.maximum(v, 0.0) + jnp.log1p(jnp.exp(-jnp.abs(v)))
    l2 = (-LOG2E) * hp_ref[:, 0:1] * dt
    r = lax.broadcasted_iota(jnp.int32, (Q, Q), 0)
    t = lax.broadcasted_iota(jnp.int32, (Q, Q), 1)
    up = (r <= t).astype(F32)
    down = (r >= t).astype(F32)
    cf = jnp.dot(l2, up, preferred_element_type=F32, precision=lax.Precision.HIGHEST)
    cb = jnp.dot(l2, down, preferred_element_type=F32, precision=lax.Precision.HIGHEST)
    forward = lax.broadcasted_iota(jnp.int32, l2.shape, 0) < heads
    cum = jnp.where(forward, cf, cb)
    total = jnp.sum(l2, axis=1, keepdims=True)
    return dt, cum, total, jnp.log2(dt) - cum


def columns_of(rows):
    used = sum(r.shape[0] for r in rows)
    if used < 128:
        rows = rows + [jnp.zeros((128 - used, Q), F32)]
    return jnp.concatenate(rows, axis=0).T


def halves(cols):
    hi = cols.astype(BF16)
    lo = (cols - hi.astype(F32)).astype(BF16)
    return jnp.concatenate([hi, lo], axis=1)


def fill_spread(spread_ref, groups, heads, width):
    for k, group in enumerate(groups):
        shape = spread_ref.shape[1:]
        j = lax.broadcasted_iota(jnp.int32, shape, 0) % 128
        head = lax.broadcasted_iota(jnp.int32, shape, 1) // width
        spread_ref[k] = jnp.where(j == group * heads + head, 1.0, 0.0).astype(BF16)


def states_kernel(
    heads, width, x_ref, bf_ref, bb_ref, raw_ref, hp_ref,
    entf_ref, entb_ref, dec_ref, end_ref, endb_ref, tot_ref, sf, sb, df, db, spread,
):
    blocks = x_ref.shape[0] // Q
    fill_spread(spread, (0, 1, 2, 3), heads, width)
    sf[...] = jnp.zeros_like(sf)
    sb[...] = jnp.zeros_like(sb)
    df[...] = jnp.ones_like(df)
    db[...] = jnp.ones_like(db)

    def step(i, _):
        k = blocks - 1 - i
        at_f = pl.multiple_of(i * Q, Q)
        at_b = pl.multiple_of(k * Q, Q)
        raw = jnp.concatenate(
            [raw_ref[:, pl.ds(at_f, Q)][:heads], raw_ref[:, pl.ds(at_b, Q)][heads:]], axis=0
        )
        _, cum, total, rowt = rates_of(raw, hp_ref, heads)
        gain = jnp.broadcast_to(jnp.exp2(total), cum.shape)
        cols = halves(columns_of([jnp.exp2(total + rowt), gain]))
        for at, block, b_ref, ent, state, dec, place in (
            (at_f, i, bf_ref, entf_ref, sf, df, 0),
            (at_b, k, bb_ref, entb_ref, sb, db, 1),
        ):
            ent[block] = state[...].astype(BF16)
            dec_ref[block, pl.ds(8 * place, 8), :] = dec[...]
            weigh = nn(cols, spread[place])
            xw = (x_ref[pl.ds(at, Q), :].astype(F32) * weigh).astype(BF16)
            decay = nn(cols[:16], spread[2 + place])[:8]
            state[...] = state[...] * decay[:1] + tn(b_ref[pl.ds(at, Q), :], xw)
            dec[...] = dec[...] * decay
        return 0

    lax.fori_loop(0, blocks, step, 0)
    end_ref[...] = sf[...].astype(BF16)
    endb_ref[...] = sb[...].astype(BF16)
    tot_ref[pl.ds(0, 8), :] = df[...]
    tot_ref[pl.ds(8, 8), :] = db[...]


def outputs_kernel(
    heads, width, x_ref, z_ref, pf_ref, pb_ref, raw_ref, hp_ref, skip_ref, gain_ref,
    entf_ref, entb_ref, dec_ref, cf_ref, cb_ref, g_ref, sq_ref, spread, base,
):
    @pl.when(pl.program_id(0) == 0)
    def _():
        fill_spread(spread, (2, 3, 5), heads, width)

    dt, cum, _, rowt = rates_of(raw_ref[...], hp_ref, heads)
    cols = columns_of([cum, jnp.exp2(cum), dt])
    b_f, c_f, b_b, c_b = pf_ref[0], pf_ref[1], pb_ref[0], pb_ref[1]
    lane = lax.broadcasted_iota(jnp.int32, (Q, 128), 1)
    diag = jnp.sum(b_b.astype(F32) * c_b.astype(F32), axis=1, keepdims=True)
    here = (lane >= 5 * heads) & (lane < 6 * heads)
    wide = halves(jnp.where(here, cols * diag + skip_ref[...], cols))
    dec = dec_ref[0]
    ent_f = (entf_ref[0].astype(F32) + dec[0:1] * cf_ref[...].astype(F32)).astype(BF16)
    ent_b = (entb_ref[0].astype(F32) + dec[8:9] * cb_ref[...].astype(F32)).astype(BF16)
    base[...] = nn(wide, spread[0]) * nn(c_f, ent_f)
    base[...] += nn(wide, spread[1]) * nn(c_b, ent_b)
    base[...] += nn(wide, spread[2]) * x_ref[...].astype(F32)

    t = lax.broadcasted_iota(jnp.int32, (Q, Q), 0)
    s = lax.broadcasted_iota(jnp.int32, (Q, Q), 1)
    lower = s <= t
    scores = jnp.where(lower, nt(c_f, b_f), nt(c_b, b_b))
    per = 128 // width
    squares = jnp.zeros((Q, 128), F32)
    for group in range(heads // per):
        lanes = slice(group * 128, (group + 1) * 128)
        x = x_ref[:, lanes]
        weights, values = [], []
        for k in range(per):
            h = group * per + k
            gap_f = cols[:, h : h + 1] + rowt[h : h + 1, :]
            gap_b = cols[:, heads + h : heads + h + 1] + rowt[heads + h : heads + h + 1, :]
            weights.append((scores * jnp.exp2(jnp.where(lower, gap_f, gap_b))).astype(BF16))
            own = (lane >= k * width) & (lane < (k + 1) * width)
            values.append(jnp.where(own, x, jnp.zeros_like(x)))
        intra = nn(jnp.concatenate(weights, axis=1), jnp.concatenate(values, axis=0))
        z = z_ref[:, lanes].astype(F32)
        gated = (base[:, lanes] + intra) * (z / (1.0 + jnp.exp(-z)))
        squares += gated * gated
        g_ref[:, lanes] = (gated * gain_ref[:, lanes]).astype(BF16)
    sums = jnp.sum(squares.T, axis=0, keepdims=True)
    sq_ref[...] = jnp.broadcast_to(sums, sq_ref.shape)


def body(
    ssm_input, gate_z, proj_forward, proj_backward, step_raw, head_params,
    skip_gain, norm_gain, out_weight,
):
    frames, inner = ssm_input.shape
    heads = step_raw.shape[1]
    width = inner // heads
    state = proj_forward.shape[2]
    blocks = frames // Q
    features = out_weight.shape[1]
    n_chan, n_seq = lax.axis_size("chan"), lax.axis_size("seq")
    chan, seq = lax.axis_index("chan"), lax.axis_index("seq")
    all_channels = inner * n_chan

    assert n_chan & (n_chan - 1) == 0

    share = inner // n_seq
    pieces = {}
    for k in range(1, n_chan):
        start = (chan ^ k) * inner + seq * share
        part = lax.dynamic_slice(out_weight, (start, 0), (share, features))
        pieces[k] = lax.ppermute(part, "chan", [(i, i ^ k) for i in range(n_chan)])
    own_weight = lax.dynamic_slice(out_weight, (chan * inner, 0), (inner, features))
    weights = {}
    for k in range(1, n_chan):
        weights[k] = [(seq * share, pieces[k])]
        for j in range(1, n_seq):
            got = lax.ppermute(pieces[k], "seq", [(i, (i + j) % n_seq) for i in range(n_seq)])
            weights[k].append((((seq + n_seq - j) % n_seq) * share, got))

    def product(gated, k):
        if k == 0:
            return jnp.dot(gated, own_weight, preferred_element_type=F32)
        return sum(
            jnp.dot(
                lax.dynamic_slice(gated, (0, at), (gated.shape[0], share)),
                part,
                preferred_element_type=F32,
            )
            for at, part in weights[k]
        )

    raw = step_raw.reshape(2 * heads, frames)
    params = jnp.stack([head_params[:, 0].reshape(-1), head_params[:, 1].reshape(-1)], axis=1)
    skip_row = jnp.zeros((1, 128), F32)
    skip_row = lax.dynamic_update_slice(skip_row, skip_gain[None], (0, 5 * heads))
    gain_row = norm_gain[None]

    states = pl.pallas_call(
        functools.partial(states_kernel, heads, width),
        out_shape=(
            jax.ShapeDtypeStruct((blocks, state, inner), BF16),
            jax.ShapeDtypeStruct((blocks, state, inner), BF16),
            jax.ShapeDtypeStruct((blocks, 16, inner), F32),
            jax.ShapeDtypeStruct((state, inner), BF16),
            jax.ShapeDtypeStruct((state, inner), BF16),
            jax.ShapeDtypeStruct((16, inner), F32),
        ),
        scratch_shapes=[
            pltpu.VMEM((state, inner), F32),
            pltpu.VMEM((state, inner), F32),
            pltpu.VMEM((8, inner), F32),
            pltpu.VMEM((8, inner), F32),
            pltpu.VMEM((4, 256, inner), BF16),
        ],
        compiler_params=pltpu.CompilerParams(vmem_limit_bytes=60 * 2**20),
        cost_estimate=pl.CostEstimate(
            flops=4 * 10**9, bytes_accessed=8 * 2**20, transcendentals=0
        ),
        name="scan_states",
    )
    ent_f, ent_b, dec, end_f, end_b, tot = states(
        ssm_input, proj_forward[0], proj_backward[0], raw, params
    )

    def carried(end, decay, step):
        pairs = [(i, i + step) for i in range(n_seq) if 0 <= i + step < n_seq]
        out = lax.ppermute(end, "seq", pairs)
        for _ in range(n_seq - 2):
            new = (end.astype(F32) + decay * out.astype(F32)).astype(BF16)
            out = lax.ppermute(new, "seq", pairs)
        return out

    carry_f = carried(end_f, tot[0:1], 1)
    carry_b = carried(end_b, tot[8:9], -1)

    chunks = next(c for c in (4, 2, 1) if blocks % c == 0)
    count = blocks // chunks
    owned, squares = [], []
    for chunk in range(chunks):
        at = chunk * count
        rows = lambda i, at=at: (i + at, 0)
        rows3 = lambda i, at=at: (0, i + at, 0)
        block3 = lambda i, at=at: (i + at, 0, 0)
        same = lambda i: (0, 0)
        outputs = pl.pallas_call(
            functools.partial(outputs_kernel, heads, width),
            grid=(count,),
            in_specs=[
                pl.BlockSpec((Q, inner), rows),
                pl.BlockSpec((Q, inner), rows),
                pl.BlockSpec((2, Q, state), rows3),
                pl.BlockSpec((2, Q, state), rows3),
                pl.BlockSpec((2 * heads, Q), lambda i, at=at: (0, i + at)),
                pl.BlockSpec((2 * heads, 2), same),
                pl.BlockSpec((1, 128), same),
                pl.BlockSpec((1, inner), same),
                pl.BlockSpec((1, state, inner), block3),
                pl.BlockSpec((1, state, inner), block3),
                pl.BlockSpec((1, 16, inner), block3),
                pl.BlockSpec((state, inner), same),
                pl.BlockSpec((state, inner), same),
            ],
            out_specs=(
                pl.BlockSpec((Q, inner), lambda i: (i, 0)),
                pl.BlockSpec((8, Q), lambda i: (0, i)),
            ),
            out_shape=(
                jax.ShapeDtypeStruct((count * Q, inner), BF16),
                jax.ShapeDtypeStruct((8, count * Q), F32),
            ),
            scratch_shapes=[pltpu.VMEM((3, 256, inner), BF16), pltpu.VMEM((Q, inner), F32)],
            compiler_params=pltpu.CompilerParams(
                vmem_limit_bytes=60 * 2**20, dimension_semantics=("arbitrary",)
            ),
            cost_estimate=pl.CostEstimate(
                flops=4 * 10**9, bytes_accessed=8 * 2**20, transcendentals=0
            ),
            name="scan_outputs",
        )
        gated, sums = outputs(
            ssm_input, gate_z, proj_forward, proj_backward, raw, params, skip_row, gain_row,
            ent_f, ent_b, dec, carry_f, carry_b,
        )
        bits = [1 << b for b in range(n_chan.bit_length() - 1)]
        bits = bits if chunk % 2 == 0 else bits[::-1]
        parts = {r: product(gated, r) for r in range(n_chan)}
        for bit in bits:
            perm = [(i, i ^ bit) for i in range(n_chan)]
            going = [r for r in parts if r & bit]
            got = jnp.concatenate([parts.pop(r).astype(BF16) for r in going], axis=0)
            got = lax.ppermute(got, "chan", perm)
            for r, part in zip(going, jnp.split(got, len(going), axis=0)):
                parts[r ^ bit] = parts[r ^ bit] + part.astype(F32)
        owned.append(parts[0])
        squares.append(sums[0:1])
    squares = jnp.concatenate(squares, axis=1)
    for bit in bits:
        perm = [(i, i ^ bit) for i in range(n_chan)]
        squares = squares + lax.ppermute(squares, "chan", perm)
    scale = lax.rsqrt(squares[0] / all_channels + 1.0)[:, None]
    received = [
        (part * scale[c * count * Q : (c + 1) * count * Q]).astype(BF16)
        for c, part in enumerate(owned)
    ]
    return jnp.concatenate(received, axis=0)


def solution(mesh):
    in_specs = (
        P(("batch", "seq"), "chan"),
        P(("batch", "seq"), "chan"),
        P(None, ("batch", "seq"), None),
        P(None, ("batch", "seq"), None),
        P(None, "chan", ("batch", "seq")),
        P(None, None, "chan"),
        P("chan"),
        P("chan"),
        P(None, "chan"),
    )
    out_specs = P(("batch", "seq"), "chan")
    return jax.shard_map(body, mesh=mesh, in_specs=in_specs, out_specs=out_specs, check_vma=False)
```

```python
import functools

import jax
import jax.numpy as jnp
from jax import lax
from jax.experimental import pallas as pl
from jax.experimental.pallas import tpu as pltpu
from jax.sharding import PartitionSpec as P


Q = 128
LOG2E = 1.4426950408889634
F32, BF16 = jnp.float32, jnp.bfloat16


def nn(a, b):
    return lax.dot_general(a, b, (((1,), (0,)), ((), ())), preferred_element_type=F32)


def nt(a, b):
    return lax.dot_general(a, b, (((1,), (1,)), ((), ())), preferred_element_type=F32)


def tn(a, b):
    return lax.dot_general(a, b, (((0,), (0,)), ((), ())), preferred_element_type=F32)


def rates_of(raw, hp_ref, heads):
    v = raw + hp_ref[:, 1:2]
    dt = jnp.maximum(v, 0.0) + jnp.log1p(jnp.exp(-jnp.abs(v)))
    l2 = (-LOG2E) * hp_ref[:, 0:1] * dt
    r = lax.broadcasted_iota(jnp.int32, (Q, Q), 0)
    t = lax.broadcasted_iota(jnp.int32, (Q, Q), 1)
    up = (r <= t).astype(F32)
    down = (r >= t).astype(F32)
    cf = jnp.dot(l2, up, preferred_element_type=F32, precision=lax.Precision.HIGHEST)
    cb = jnp.dot(l2, down, preferred_element_type=F32, precision=lax.Precision.HIGHEST)
    forward = lax.broadcasted_iota(jnp.int32, l2.shape, 0) < heads
    cum = jnp.where(forward, cf, cb)
    total = jnp.sum(l2, axis=1, keepdims=True)
    return dt, cum, total, jnp.log2(dt) - cum


def columns_of(rows):
    used = sum(r.shape[0] for r in rows)
    if used < 128:
        rows = rows + [jnp.zeros((128 - used, Q), F32)]
    return jnp.concatenate(rows, axis=0).T


def halves(cols):
    hi = cols.astype(BF16)
    lo = (cols - hi.astype(F32)).astype(BF16)
    return jnp.concatenate([hi, lo], axis=1)


def fill_spread(spread_ref, groups, heads, width):
    for k, group in enumerate(groups):
        shape = spread_ref.shape[1:]
        j = lax.broadcasted_iota(jnp.int32, shape, 0) % 128
        head = lax.broadcasted_iota(jnp.int32, shape, 1) // width
        spread_ref[k] = jnp.where(j == group * heads + head, 1.0, 0.0).astype(BF16)


def states_kernel(
    heads, width, x_ref, bf_ref, bb_ref, raw_ref, hp_ref,
    entf_ref, entb_ref, dec_ref, end_ref, endb_ref, tot_ref, sf, sb, df, db, spread,
):
    blocks = x_ref.shape[0] // Q
    fill_spread(spread, (0, 1, 2, 3), heads, width)
    sf[...] = jnp.zeros_like(sf)
    sb[...] = jnp.zeros_like(sb)
    df[...] = jnp.ones_like(df)
    db[...] = jnp.ones_like(db)

    def step(i, _):
        k = blocks - 1 - i
        at_f = pl.multiple_of(i * Q, Q)
        at_b = pl.multiple_of(k * Q, Q)
        raw = jnp.concatenate(
            [raw_ref[:, pl.ds(at_f, Q)][:heads], raw_ref[:, pl.ds(at_b, Q)][heads:]], axis=0
        )
        _, cum, total, rowt = rates_of(raw, hp_ref, heads)
        gain = jnp.broadcast_to(jnp.exp2(total), cum.shape)
        cols = halves(columns_of([jnp.exp2(total + rowt), gain]))
        for at, block, b_ref, ent, state, dec, place in (
            (at_f, i, bf_ref, entf_ref, sf, df, 0),
            (at_b, k, bb_ref, entb_ref, sb, db, 1),
        ):
            ent[block] = state[...].astype(BF16)
            dec_ref[block, pl.ds(8 * place, 8), :] = dec[...]
            weigh = nn(cols, spread[place])
            xw = (x_ref[pl.ds(at, Q), :].astype(F32) * weigh).astype(BF16)
            decay = nn(cols[:16], spread[2 + place])[:8]
            state[...] = state[...] * decay[:1] + tn(b_ref[0, pl.ds(at, Q), :], xw)
            dec[...] = dec[...] * decay
        return 0

    lax.fori_loop(0, blocks, step, 0)
    end_ref[...] = sf[...].astype(BF16)
    endb_ref[...] = sb[...].astype(BF16)
    tot_ref[pl.ds(0, 8), :] = df[...]
    tot_ref[pl.ds(8, 8), :] = db[...]


def outputs_kernel(
    heads, width, x_ref, z_ref, pf_ref, pb_ref, raw_ref, hp_ref, skip_ref, gain_ref,
    entf_ref, entb_ref, dec_ref, cf_ref, cb_ref, g_ref, sq_ref, spread, base,
):
    @pl.when(pl.program_id(0) == 0)
    def _():
        fill_spread(spread, (2, 3, 5), heads, width)

    dt, cum, _, rowt = rates_of(raw_ref[...], hp_ref, heads)
    cols = columns_of([cum, jnp.exp2(cum), dt])
    b_f, c_f, b_b, c_b = pf_ref[0], pf_ref[1], pb_ref[0], pb_ref[1]
    lane = lax.broadcasted_iota(jnp.int32, (Q, 128), 1)
    diag = jnp.sum(b_b.astype(F32) * c_b.astype(F32), axis=1, keepdims=True)
    here = (lane >= 5 * heads) & (lane < 6 * heads)
    wide = halves(jnp.where(here, cols * diag + skip_ref[...], cols))
    dec = dec_ref[0]
    ent_f = (entf_ref[0].astype(F32) + dec[0:1] * cf_ref[...].astype(F32)).astype(BF16)
    ent_b = (entb_ref[0].astype(F32) + dec[8:9] * cb_ref[...].astype(F32)).astype(BF16)
    base[...] = nn(wide, spread[0]) * nn(c_f, ent_f)
    base[...] += nn(wide, spread[1]) * nn(c_b, ent_b)
    base[...] += nn(wide, spread[2]) * x_ref[...].astype(F32)

    t = lax.broadcasted_iota(jnp.int32, (Q, Q), 0)
    s = lax.broadcasted_iota(jnp.int32, (Q, Q), 1)
    lower = s <= t
    scores = jnp.where(lower, nt(c_f, b_f), nt(c_b, b_b))
    per = 128 // width
    squares = jnp.zeros((Q, 128), F32)
    for group in range(heads // per):
        lanes = slice(group * 128, (group + 1) * 128)
        x = x_ref[:, lanes]
        weights, values = [], []
        for k in range(per):
            h = group * per + k
            gap_f = cols[:, h : h + 1] + rowt[h : h + 1, :]
            gap_b = cols[:, heads + h : heads + h + 1] + rowt[heads + h : heads + h + 1, :]
            weights.append((scores * jnp.exp2(jnp.where(lower, gap_f, gap_b))).astype(BF16))
            own = (lane >= k * width) & (lane < (k + 1) * width)
            values.append(jnp.where(own, x, jnp.zeros_like(x)))
        intra = nn(jnp.concatenate(weights, axis=1), jnp.concatenate(values, axis=0))
        z = z_ref[:, lanes].astype(F32)
        gated = (base[:, lanes] + intra) * (z / (1.0 + jnp.exp(-z)))
        squares += gated * gated
        g_ref[:, lanes] = (gated * gain_ref[:, lanes]).astype(BF16)
    sums = jnp.sum(squares.T, axis=0, keepdims=True)
    sq_ref[...] = jnp.broadcast_to(sums, sq_ref.shape)


def body(
    ssm_input, gate_z, proj_forward, proj_backward, step_raw, head_params,
    skip_gain, norm_gain, out_weight,
):
    frames, inner = ssm_input.shape
    heads = step_raw.shape[1]
    width = inner // heads
    state = proj_forward.shape[2]
    blocks = frames // Q
    features = out_weight.shape[1]
    n_chan, n_seq = lax.axis_size("chan"), lax.axis_size("seq")
    chan, seq = lax.axis_index("chan"), lax.axis_index("seq")
    all_channels = inner * n_chan

    assert n_chan & (n_chan - 1) == 0

    share = inner // n_seq
    pieces = {}
    for k in range(1, n_chan):
        start = (chan ^ k) * inner + seq * share
        part = lax.dynamic_slice(out_weight, (start, 0), (share, features))
        pieces[k] = lax.ppermute(part, "chan", [(i, i ^ k) for i in range(n_chan)])
    own_weight = lax.dynamic_slice(out_weight, (chan * inner, 0), (inner, features))
    weights = {}
    for k in range(1, n_chan):
        weights[k] = [(seq * share, pieces[k])]
        for j in range(1, n_seq):
            got = lax.ppermute(pieces[k], "seq", [(i, (i + j) % n_seq) for i in range(n_seq)])
            weights[k].append((((seq + n_seq - j) % n_seq) * share, got))

    def product(gated, k):
        if k == 0:
            return jnp.dot(gated, own_weight, preferred_element_type=F32)
        return sum(
            jnp.dot(
                lax.dynamic_slice(gated, (0, at), (gated.shape[0], share)),
                part,
                preferred_element_type=F32,
            )
            for at, part in weights[k]
        )

    raw = step_raw.reshape(2 * heads, frames)
    params = jnp.stack([head_params[:, 0].reshape(-1), head_params[:, 1].reshape(-1)], axis=1)
    skip_row = jnp.zeros((1, 128), F32)
    skip_row = lax.dynamic_update_slice(skip_row, skip_gain[None], (0, 5 * heads))
    gain_row = norm_gain[None]

    states = pl.pallas_call(
        functools.partial(states_kernel, heads, width),
        out_shape=(
            jax.ShapeDtypeStruct((blocks, state, inner), BF16),
            jax.ShapeDtypeStruct((blocks, state, inner), BF16),
            jax.ShapeDtypeStruct((blocks, 16, inner), F32),
            jax.ShapeDtypeStruct((state, inner), BF16),
            jax.ShapeDtypeStruct((state, inner), BF16),
            jax.ShapeDtypeStruct((16, inner), F32),
        ),
        scratch_shapes=[
            pltpu.VMEM((state, inner), F32),
            pltpu.VMEM((state, inner), F32),
            pltpu.VMEM((8, inner), F32),
            pltpu.VMEM((8, inner), F32),
            pltpu.VMEM((4, 256, inner), BF16),
        ],
        compiler_params=pltpu.CompilerParams(vmem_limit_bytes=60 * 2**20),
        cost_estimate=pl.CostEstimate(
            flops=4 * 10**9, bytes_accessed=8 * 2**20, transcendentals=0
        ),
        name="scan_states",
    )
    ent_f, ent_b, dec, end_f, end_b, tot = states(
        ssm_input, proj_forward, proj_backward, raw, params
    )

    def carried(end, decay, step):
        pairs = [(i, i + step) for i in range(n_seq) if 0 <= i + step < n_seq]
        out = lax.ppermute(end, "seq", pairs)
        for _ in range(n_seq - 2):
            new = (end.astype(F32) + decay * out.astype(F32)).astype(BF16)
            out = lax.ppermute(new, "seq", pairs)
        return out

    carry_f = carried(end_f, tot[0:1], 1)
    carry_b = carried(end_b, tot[8:9], -1)

    chunks = next(c for c in (4, 2, 1) if blocks % c == 0)
    count = blocks // chunks
    owned, squares = [], []
    for chunk in range(chunks):
        at = chunk * count
        rows = lambda i, at=at: (i + at, 0)
        rows3 = lambda i, at=at: (0, i + at, 0)
        block3 = lambda i, at=at: (i + at, 0, 0)
        same = lambda i: (0, 0)
        outputs = pl.pallas_call(
            functools.partial(outputs_kernel, heads, width),
            grid=(count,),
            in_specs=[
                pl.BlockSpec((Q, inner), rows),
                pl.BlockSpec((Q, inner), rows),
                pl.BlockSpec((2, Q, state), rows3),
                pl.BlockSpec((2, Q, state), rows3),
                pl.BlockSpec((2 * heads, Q), lambda i, at=at: (0, i + at)),
                pl.BlockSpec((2 * heads, 2), same),
                pl.BlockSpec((1, 128), same),
                pl.BlockSpec((1, inner), same),
                pl.BlockSpec((1, state, inner), block3),
                pl.BlockSpec((1, state, inner), block3),
                pl.BlockSpec((1, 16, inner), block3),
                pl.BlockSpec((state, inner), same),
                pl.BlockSpec((state, inner), same),
            ],
            out_specs=(
                pl.BlockSpec((Q, inner), lambda i: (i, 0)),
                pl.BlockSpec((8, Q), lambda i: (0, i)),
            ),
            out_shape=(
                jax.ShapeDtypeStruct((count * Q, inner), BF16),
                jax.ShapeDtypeStruct((8, count * Q), F32),
            ),
            scratch_shapes=[pltpu.VMEM((3, 256, inner), BF16), pltpu.VMEM((Q, inner), F32)],
            compiler_params=pltpu.CompilerParams(
                vmem_limit_bytes=60 * 2**20, dimension_semantics=("arbitrary",)
            ),
            cost_estimate=pl.CostEstimate(
                flops=4 * 10**9, bytes_accessed=8 * 2**20, transcendentals=0
            ),
            name="scan_outputs",
        )
        gated, sums = outputs(
            ssm_input, gate_z, proj_forward, proj_backward, raw, params, skip_row, gain_row,
            ent_f, ent_b, dec, carry_f, carry_b,
        )
        bits = [1 << b for b in range(n_chan.bit_length() - 1)]
        bits = bits if chunk % 2 == 0 else bits[::-1]
        parts = {r: product(gated, r) for r in range(n_chan)}
        for bit in bits:
            perm = [(i, i ^ bit) for i in range(n_chan)]
            going = [r for r in parts if r & bit]
            got = jnp.concatenate([parts.pop(r).astype(BF16) for r in going], axis=0)
            got = lax.ppermute(got, "chan", perm)
            for r, part in zip(going, jnp.split(got, len(going), axis=0)):
                parts[r ^ bit] = parts[r ^ bit] + part.astype(F32)
        owned.append(parts[0])
        squares.append(sums)
    squares = jnp.concatenate(squares, axis=1)
    for bit in bits:
        perm = [(i, i ^ bit) for i in range(n_chan)]
        squares = squares + lax.ppermute(squares, "chan", perm)
    scale = lax.rsqrt(squares[0] / all_channels + 1.0)[:, None]
    received = [
        (part * scale[c * count * Q : (c + 1) * count * Q]).astype(BF16)
        for c, part in enumerate(owned)
    ]
    return jnp.concatenate(received, axis=0)


def solution(mesh):
    in_specs = (
        P(("batch", "seq"), "chan"),
        P(("batch", "seq"), "chan"),
        P(None, ("batch", "seq"), None),
        P(None, ("batch", "seq"), None),
        P(None, "chan", ("batch", "seq")),
        P(None, None, "chan"),
        P("chan"),
        P("chan"),
        P(None, "chan"),
    )
    out_specs = P(("batch", "seq"), "chan")
    return jax.shard_map(body, mesh=mesh, in_specs=in_specs, out_specs=out_specs, check_vma=False)
```
